32 devices in a mesh: row: 16 (over z, y, core), col: 2 (over x).
Axes of the slice: x: 2, y: 2, z: 4, core: 2. Of those that a mesh axis runs over, the one named last changes fastest.
Arguments:
- hidden: bfloat16 [4096, 768], P(('row', 'col')), may hold values from -6 to 6
- projection: bfloat16 [768, 512], replicated, may hold values from -0.21875 to 0.21875
- alpha: bfloat16 [4096], P(('row', 'col')), may hold values from -6 to 6
- probe_pairs: bfloat16 [4096, 32], P(('row', 'col')), may hold values from -6 to 6
- amplitude: float32 [1], replicated, may hold values from 0.5 to 2
- length_sq: float32 [1], replicated, may hold values from 512 to 1024
Outputs:
- grad_hidden: bfloat16 [4096, 768], P(('row', 'col'))
- grad_proj: float32 [768, 512], P('row')
The draws below stay inside these ranges and needn't reach their ends.
All inputs are finite; a program needn't handle non-finite values.
Results may differ from the reference program's by a relative error of at most 0.023.
Values may be sent and summed in bfloat16 or wider, within the bound.
A program may use at most 64 MiB of HBM per device.

```python
import math
import jax
import jax.numpy as jnp
from jax import lax

HID = 768
FEAT = 512
PROBES = 16
POINTS = 4096
N_ROW = 16


def draw_hidden(key, part):
    groups = max(POINTS // 256, 2)
    centers = jax.random.normal(jax.random.fold_in(key, 13), (groups, HID), jnp.float32)
    labels = jax.random.randint(jax.random.fold_in(key, 14), (POINTS,), 0, groups)
    placed = 2.0 * jnp.take(centers, labels, axis=0)
    values = placed + jax.random.normal(jax.random.fold_in(key, 11), (POINTS, HID), jnp.float32)
    values = jnp.clip(values, -6.0, 6.0)
    return values.astype(jnp.bfloat16)


def level_of(key, extent, pieces, smallest, top_value):
    loudness, own = 1.0, jax.random.fold_in(key, 6)
    for dim, blocks in pieces:
        heights = jnp.exp(jax.random.uniform(jax.random.fold_in(own, dim), (blocks,), jnp.float32, smallest / len(pieces), top_value / len(pieces)))
        loudness = loudness * jnp.repeat(heights, extent[dim] // blocks).reshape([-1 if axis == dim else 1 for axis in range(len(extent))])
    return loudness


def bell_draw(own_key, extent, width, bound, pieces=(), held_as=jnp.bfloat16):
    entries = width * jax.random.normal(own_key, extent, jnp.float32)
    if pieces:
        entries = entries * level_of(own_key, extent, pieces, -0.22, 0.18)
    return jnp.clip(entries, -bound, bound).astype(held_as)


def setup_inputs(seed: int = 0) -> dict:
    key_of = jax.random.split(jax.random.key(seed), 7)
    return {
        "hidden": draw_hidden(jax.random.fold_in(key_of[6], 71), 0),
        "projection": bell_draw(key_of[1], (HID, FEAT), HID ** -0.5, 0.21875),
        "alpha": bell_draw(key_of[2], (POINTS,), 1.0, 6.0, ((0, 32),)),
        "probe_pairs": bell_draw(key_of[3], (POINTS, 2 * PROBES), 1.0, 6.0, ((0, 32),)),
        "amplitude": jnp.clip(jnp.exp(jax.random.uniform(key_of[4], (1,), jnp.float32, math.log(0.5), math.log(2.0))), 0.5, 2.0),
        "length_sq": jnp.clip(jnp.exp(jax.random.uniform(key_of[5], (1,), jnp.float32, math.log(512.0), math.log(1024.0))), 512.0, 1024.0),
    }


def right_of(factors, probes):
    scale = 1.0 / (4 * probes)
    return jnp.concatenate([factors[:, :1] * 0.5, factors[:, 1 + probes:] * (-scale), factors[:, 1:1 + probes] * (-scale)], axis=1)


def reference(hidden, projection, alpha, probe_pairs, amplitude, length_sq):
    feats = jnp.dot(hidden, projection, preferred_element_type=jnp.float32).astype(jnp.bfloat16)
    left = jnp.concatenate([alpha[:, None], probe_pairs], axis=1)
    probes = probe_pairs.shape[1] // 2
    right = right_of(left, probes)
    amp = amplitude[0]
    lsq = length_sq[0]
    feat_f = feats.astype(jnp.float32)
    sq_all = jnp.sum(feat_f * feat_f, axis=1)
    block = POINTS // N_ROW

    def one_block(index):
        start = (index * block).astype(jnp.int32)
        rows_feat = lax.dynamic_slice_in_dim(feats, start, block, 0)
        rows_left = lax.dynamic_slice_in_dim(left, start, block, 0)
        rows_sq = lax.dynamic_slice_in_dim(sq_all, start, block, 0)
        inner = jnp.dot(rows_feat, feats.T, preferred_element_type=jnp.float32)
        dist = rows_sq[:, None] + sq_all[None, :] - 2.0 * inner
        kern = amp * jnp.exp(-0.5 * dist / lsq)
        gmat = jnp.dot(rows_left, right.T, preferred_element_type=jnp.float32)
        weight = gmat * kern
        rowsum = jnp.sum(weight, axis=1)
        moved = jnp.dot(weight.astype(jnp.bfloat16), feats, preferred_element_type=jnp.float32)
        return moved, rowsum

    moved, rowsum = lax.map(one_block, jnp.arange(N_ROW, dtype=jnp.int32))
    moved = moved.reshape(POINTS, -1)
    rowsum = rowsum.reshape(POINTS)
    grad_feat = ((2.0 / lsq) * (moved - rowsum[:, None] * feat_f)).astype(jnp.bfloat16)
    grad_hidden = jnp.dot(grad_feat, projection.T, preferred_element_type=jnp.float32).astype(jnp.bfloat16)
    grad_proj = lax.dot_general(hidden, grad_feat, (((0,), (0,)), ((), ())), preferred_element_type=jnp.float32)
    return grad_hidden, grad_proj
```

```python
import functools
import math

import jax
import jax.numpy as jnp
from jax import lax
from jax.experimental import pallas as pl
from jax.experimental.pallas import tpu as pltpu
from jax.sharding import PartitionSpec as P


def right_of(factors, probes):
    scale = 1.0 / (4 * probes)
    return jnp.concatenate(
        [
            factors[:, :1] * 0.5,
            factors[:, 1 + probes :] * -scale,
            factors[:, 1 : 1 + probes] * -scale,
        ],
        axis=1,
    )


def squares(feats):
    feat_f = feats.astype(jnp.float32)
    return jnp.sum(feat_f * feat_f, axis=1)


def per_device(hidden, projection, alpha, probe_pairs, amplitude, length_sq):
    feats = jnp.dot(hidden, projection, preferred_element_type=jnp.float32).astype(jnp.bfloat16)
    factors = jnp.concatenate([alpha[:, None], probe_pairs], axis=1)
    probes = probe_pairs.shape[1] // 2
    amp = amplitude[0]
    lsq = length_sq[0]
    width = feats.shape[1]

    def make_fold(rows_feat, rows_fac):
        rows_sq = squares(rows_feat)

        def fold(carry, pieces, start):
            cols_feat, cols_fac = pieces
            count = cols_feat.shape[0]
            size = math.gcd(count, 256)
            steps_feat = cols_feat.reshape(count // size, size, width)
            steps_fac = cols_fac.reshape(count // size, size, cols_fac.shape[1])

            def inner_step(state, blocks):
                block_feat, block_fac = blocks
                moved, rowsum = state
                block_sq = squares(block_feat)
                inner = jnp.dot(rows_feat, block_feat.T, preferred_element_type=jnp.float32)
                dist = rows_sq[:, None] + block_sq[None, :] - 2.0 * inner
                kern = amp * jnp.exp(-0.5 * dist / lsq)
                gmat = jnp.dot(
                    rows_fac, right_of(block_fac, probes).T, preferred_element_type=jnp.float32
                )
                weight = gmat * kern
                rowsum = rowsum + jnp.sum(weight, axis=1)
                moved = moved + jnp.dot(
                    weight.astype(jnp.bfloat16), block_feat, preferred_element_type=jnp.float32
                )
                return ((moved, rowsum), None)

            result, unused = lax.scan(inner_step, carry, (steps_feat, steps_fac))
            return result

        start_carry = (
            jnp.zeros((rows_feat.shape[0], width), jnp.float32),
            jnp.zeros((rows_feat.shape[0],), jnp.float32),
        )
        return (fold, start_carry)

    rows_feat, rows_fac = (
        lax.all_gather(feats, "row", axis=0, tiled=True),
        lax.all_gather(factors, "row", axis=0, tiled=True),
    )
    fold, start_carry = make_fold(rows_feat, rows_fac)
    moved, rowsum = fold(
        start_carry,
        (
            lax.all_gather(feats, "col", axis=0, tiled=True),
            lax.all_gather(factors, "col", axis=0, tiled=True),
        ),
        jnp.int32(0),
    )
    moved_own, rowsum_own = (
        lax.psum_scatter(moved, "row", scatter_dimension=0, tiled=True),
        lax.psum_scatter(rowsum, "row", scatter_dimension=0, tiled=True),
    )
    grad_feat = (2.0 / lsq * (moved_own - rowsum_own[:, None] * feats.astype(jnp.float32))).astype(
        jnp.bfloat16
    )
    grad_hidden = jnp.dot(grad_feat, projection.T, preferred_element_type=jnp.float32).astype(
        jnp.bfloat16
    )
    partial_proj = lax.dot_general(
        hidden, grad_feat, (((0,), (0,)), ((), ())), preferred_element_type=jnp.float32
    )
    share = lax.psum_scatter(
        partial_proj.astype(jnp.bfloat16), "row", scatter_dimension=0, tiled=True
    )
    grad_proj = lax.psum(share, "col").astype(jnp.float32)
    return (grad_hidden, grad_proj)


TILE = 16
LANES = 128
MESH = pl.DeviceIdType.MESH
NT = (((1,), (1,)), ((), ()))


def fused_kernel(
    n_q,
    hidden,
    proj,
    fac,
    amp,
    lsq,
    gh_ref,
    gp_ref,
    blocks,
    rows_blk,
    rows_fac,
    rows_hid,
    row_sq,
    hid_t,
    moved,
    rowsum,
    part_d,
    peer_d,
    grad,
    y_out,
    y_in,
    q_out,
    q_in,
    x_out,
    x_in,
    send_sems,
    recv_sems,
    core_send,
    core_recv,
    y_send,
    y_recv,
    q_send,
    q_recv,
    x_send,
    x_recv,
):
    r = lax.axis_index("row")
    c = lax.axis_index("col")
    k = lax.rem(r, 2)
    y = lax.rem(r // 2, 2)
    q = r // 4
    pts, hid = hidden.shape
    feat = proj.shape[1]
    share = gp_ref.shape[0]
    mid = pts // 2

    def dev(qq, yy, cc, kk):
        return ((qq * 2 + yy) * 2 + kk, cc)

    y_nbr = dev(q, 1 - y, c, k)
    c_nbr = dev(q, y, 1 - c, k)
    core = dev(q, y, c, 1 - k)
    q_up = dev(jnp.minimum(q + 1, n_q - 1), y, c, k)
    q_dn = dev(jnp.maximum(q - 1, 0), y, c, k)

    barrier = pltpu.get_barrier_semaphore()
    for nbr in (y_nbr, c_nbr, core):
        pl.semaphore_signal(barrier, inc=1, device_id=nbr, device_id_type=MESH)
    for i in range(1, n_q):
        pl.semaphore_signal(
            barrier, inc=1, device_id=dev(lax.rem(q + i, n_q), y, c, k), device_id_type=MESH
        )

    def slot_of(oq, oy, oc):
        return (oq * 2 + oy) * 2 + oc

    mine = slot_of(q, y, c)

    feats = jnp.dot(hidden[...], proj[...], preferred_element_type=jnp.float32).astype(jnp.bfloat16)
    feat_f = feats.astype(jnp.float32)
    sq = lax.dot_general(
        jnp.ones((8, feat), jnp.float32),
        feat_f * feat_f,
        NT,
        precision=lax.Precision.HIGHEST,
        preferred_element_type=jnp.float32,
    )
    sq = jnp.concatenate([sq, sq], axis=0)
    hi = sq.astype(jnp.bfloat16).astype(jnp.float32)
    mi = (sq - hi).astype(jnp.bfloat16).astype(jnp.float32)
    lo = sq - hi - mi
    fac_t = fac[:, :LANES].astype(jnp.float32).T
    place = lax.broadcasted_iota(jnp.int32, (TILE, pts), 0)
    last = fac_t[2 * TILE : 3 * TILE]
    last = jnp.where(place == 1, hi, jnp.where(place == 2, mi, jnp.where(place == 3, lo, last)))
    blocks[mine, 0:pts, :] = feats
    rows_blk[k] = feats
    blocks[mine, pts:, :] = jnp.zeros((TILE, feat), jnp.bfloat16)
    blocks[mine, pts:, 0:pts] = fac_t[0:TILE].astype(jnp.bfloat16)
    blocks[mine, pts:, pts : 2 * pts] = fac_t[TILE : 2 * TILE].astype(jnp.bfloat16)
    blocks[mine, pts:, 2 * pts : 3 * pts] = last.astype(jnp.bfloat16)
    rows_fac[k] = fac[:, LANES:]

    pl.semaphore_wait(barrier, 3 + n_q - 1)

    def to_core(index, src, dst):
        return pltpu.make_async_remote_copy(
            src_ref=src,
            dst_ref=dst,
            send_sem=core_send.at[index],
            recv_sem=core_recv.at[index],
            device_id=core,
            device_id_type=MESH,
        )

    first = (
        to_core(0, blocks.at[mine, 0:pts], rows_blk.at[k]),
        to_core(1, fac.at[:, LANES : 2 * LANES], rows_fac.at[k]),
        to_core(2, hidden, rows_hid),
    )

    spans = ((0, mid), (mid, pts + TILE - mid))

    def hop(direction, part, slot, nbr):
        piece = blocks.at[slot, pl.ds(*spans[part])]
        return pltpu.make_async_remote_copy(
            src_ref=piece,
            dst_ref=piece,
            send_sem=send_sems.at[direction, part, slot],
            recv_sem=recv_sems.at[part, slot],
            device_id=nbr,
            device_id_type=MESH,
        )

    sent = []

    def send(pred, copy):
        sent.append((pred, copy))
        if pred is None:
            copy.start()
        else:
            pl.when(pred)(copy.start)

    def both(a, b):
        return b if a is None else jnp.logical_and(a, b)

    def forward(exists, part, oq, iy, ic, own=False):
        slot = slot_of(oq, (y + iy) % 2, (c + ic) % 2)
        if not own:
            arrival = hop(0, part, slot, y_nbr)
            pl.when(exists)(arrival.wait_recv)
        if part == 0:
            if iy == 0 and ic == 0:
                send(exists, hop(3, part, slot, c_nbr))
            if iy == 0:
                send(exists, hop(2, part, slot, y_nbr))
        else:
            if iy == 0 and ic == 0:
                send(exists, hop(2, part, slot, y_nbr))
            if ic == 0:
                send(exists, hop(3, part, slot, c_nbr))

    def forward_q(exists, part, oq):
        slot = slot_of(oq, y, c)
        up = jnp.logical_and(oq <= q, q + 1 < n_q)
        down = jnp.logical_and(oq >= q, q > 0)
        send(both(exists, up), hop(0, part, slot, q_up))
        send(both(exists, down), hop(1, part, slot, q_dn))

    scale = -0.5 / lsq[0]

    def fold(slot):
        blk = blocks[slot, 0:pts, :]
        aux = blocks[slot, pts:, :]
        rows = jnp.concatenate([rows_blk[0], rows_blk[1]], axis=0)
        inner = lax.dot_general(rows, blk, NT, preferred_element_type=jnp.float32)
        tail = aux[:, 2 * pts : 3 * pts].astype(jnp.float32)
        col_sq = tail[1:2] + tail[2:3] + tail[3:4]
        dist = row_sq[...] + col_sq - 2.0 * inner
        kern = jnp.exp(dist * scale)
        col_fac = jnp.concatenate(
            [
                aux[:, 0:pts],
                aux[:, pts : 2 * pts],
                aux[:, 2 * pts : 3 * pts],
                jnp.zeros((LANES - 3 * TILE, pts), jnp.bfloat16),
            ],
            axis=0,
        )
        lefts = jnp.concatenate([rows_fac[0], rows_fac[1]], axis=0)
        gmat = jnp.dot(lefts, col_fac, preferred_element_type=jnp.float32)
        weight = gmat * kern
        rowsum[...] += weight
        moved[...] += jnp.dot(weight.astype(jnp.bfloat16), blk, preferred_element_type=jnp.float32)

    def fold_level(level):
        def step(e, carry):
            iy, ic, side = e // 4, lax.rem(e // 2, 2), lax.rem(e, 2)
            dq = level - iy - ic
            oq = q + dq * (1 - 2 * side)
            good = (dq >= 0) & (dq < n_q) & (oq >= 0) & (oq < n_q) & ((dq > 0) | (side == 0))

            @pl.when(good)
            def _():
                fold(slot_of(oq, lax.rem(y + iy, 2), lax.rem(c + ic, 2)))

            return carry

        lax.fori_loop(0, 8, step, 0)

    for level in range(n_q + 2):
        if level == 0:
            for part in (0, 1):
                forward(None, part, q, 0, 0, own=True)
                forward_q(None, part, q)
            for copy in first:
                copy.start()
            for copy in first:
                copy.wait_recv()
            for half in range(2):
                f = rows_blk[half].astype(jnp.float32)
                row_sq[half * pts : (half + 1) * pts, :] = jnp.broadcast_to(
                    jnp.sum(f * f, axis=1, keepdims=True), (pts, pts)
                )
            moved[...] = jnp.zeros_like(moved)
            rowsum[...] = jnp.zeros_like(rowsum)
        for iy, ic in ((0, 0), (0, 1), (1, 0), (1, 1)):
            dq = level - iy - ic
            if dq < 0 or dq >= n_q or level == 0:
                continue
            for side in (1, -1) if dq else (1,):
                oq = q + side * dq
                exists = None if dq == 0 else jnp.logical_and(oq >= 0, oq < n_q)
                if exists is None:
                    exists = q >= 0
                for part in (0, 1):
                    forward(exists, part, oq, iy, ic)
                    if iy == 0 and ic == 0:
                        forward_q(exists, part, oq)
        fold_level(level)
        if level == 0:
            own_t = hidden[...].astype(jnp.float32).T.astype(jnp.bfloat16)
            peer_t = rows_hid[...].astype(jnp.float32).T.astype(jnp.bfloat16)
            low = k == 0
            hid_t[:, 0:pts] = jnp.where(low, own_t, peer_t)
            hid_t[:, pts:] = jnp.where(low, peer_t, own_t)

    rows_f = jnp.concatenate([rows_blk[0], rows_blk[1]], axis=0).astype(jnp.float32)
    part_d[...] = moved[...] - jnp.sum(rowsum[...], axis=1, keepdims=True) * rows_f
    swap = to_core(3, part_d, peer_d)
    swap.start()
    swap.wait_recv()
    grad[...] = ((2.0 * amp[0] / lsq[0]) * (part_d[...] + peer_d[...])).astype(jnp.bfloat16)

    def term(qj, yj):
        start = pl.multiple_of(((qj * 2 + yj) * 2 + k) * share, TILE)
        return jnp.dot(hid_t[pl.ds(start, share), :], grad[...], preferred_element_type=jnp.float32)

    def to_y(qj):
        return pltpu.make_async_remote_copy(
            src_ref=y_out.at[qj],
            dst_ref=y_in.at[qj],
            send_sem=y_send.at[qj],
            recv_sem=y_recv.at[qj],
            device_id=y_nbr,
            device_id_type=MESH,
        )

    def to_q(qj):
        return pltpu.make_async_remote_copy(
            src_ref=q_out.at[qj],
            dst_ref=q_in.at[q],
            send_sem=q_send.at[qj],
            recv_sem=q_recv.at[q],
            device_id=dev(qj, y, c, k),
            device_id_type=MESH,
        )

    def from_q(qj):
        return pltpu.make_async_remote_copy(
            src_ref=q_out.at[qj],
            dst_ref=q_in.at[qj],
            send_sem=q_send.at[qj],
            recv_sem=q_recv.at[qj],
            device_id=dev(qj, y, c, k),
            device_id_type=MESH,
        )

    order = [lax.rem(q + i, n_q) for i in range(1, n_q)] + [q]
    for qj in order:
        y_out[qj] = term(qj, 1 - y).astype(jnp.bfloat16)
        to_y(qj).start()
    own_rows = grad[pl.ds(pl.multiple_of(k * pts, pts), pts), :]
    gh_ref[...] = lax.dot_general(
        own_rows, proj[...], NT, preferred_element_type=jnp.float32
    ).astype(jnp.bfloat16)
    total = None
    for qj in order:
        own_term = term(qj, y)
        to_y(qj).wait_recv()
        summed = own_term + y_in[qj].astype(jnp.float32)
        if qj is order[-1]:
            total = summed
        else:
            q_out[qj] = summed.astype(jnp.bfloat16)
            to_q(qj).start()
    for qj in order[:-1]:
        from_q(qj).wait_recv()
        total = total + q_in[qj].astype(jnp.float32)
    x_out[...] = total.astype(jnp.bfloat16)
    to_x = pltpu.make_async_remote_copy(
        src_ref=x_out,
        dst_ref=x_in,
        send_sem=x_send,
        recv_sem=x_recv,
        device_id=c_nbr,
        device_id_type=MESH,
    )
    to_x.start()
    to_x.wait_recv()
    gp_ref[...] = x_out[...].astype(jnp.float32) + x_in[...].astype(jnp.float32)

    for pred, copy in sent:
        if pred is None:
            copy.wait_send()
        else:
            pl.when(pred)(copy.wait_send)
    for copy in first:
        copy.wait_send()
    swap.wait_send()
    for qj in order:
        to_y(qj).wait_send()
    for qj in order[:-1]:
        to_q(qj).wait_send()
    to_x.wait_send()


def fused(n_row, n_col, hidden, projection, alpha, probe_pairs, amplitude, length_sq):
    pts, hid = hidden.shape
    feat = projection.shape[1]
    probes = probe_pairs.shape[1] // 2
    slots = n_row * n_col // 2
    n_q = n_row // 4
    share = hid // n_row
    step = 1.0 / (4 * probes)
    fill = jnp.zeros((pts, LANES - 2 * probes - 1), jnp.bfloat16)
    fac = jnp.concatenate(
        [
            probe_pairs,
            alpha[:, None],
            fill,
            probe_pairs[:, probes:] * -step,
            probe_pairs[:, :probes] * -step,
            alpha[:, None] * 0.5,
            fill,
        ],
        axis=1,
    )
    vmem = pl.BlockSpec(memory_space=pltpu.VMEM)
    smem = pl.BlockSpec(memory_space=pltpu.SMEM)
    bf, f32 = jnp.bfloat16, jnp.float32
    dma = pltpu.SemaphoreType.DMA
    return pl.pallas_call(
        functools.partial(fused_kernel, n_q),
        out_shape=(
            jax.ShapeDtypeStruct((pts, hid), bf),
            jax.ShapeDtypeStruct((share, feat), f32),
        ),
        in_specs=[vmem, vmem, vmem, smem, smem],
        out_specs=(vmem, vmem),
        scratch_shapes=[
            pltpu.VMEM((slots, pts + TILE, feat), bf),
            pltpu.VMEM((2, pts, feat), bf),
            pltpu.VMEM((2, pts, LANES), bf),
            pltpu.VMEM((pts, hid), bf),
            pltpu.VMEM((2 * pts, pts), f32),
            pltpu.VMEM((hid, 2 * pts), bf),
            pltpu.VMEM((2 * pts, feat), f32),
            pltpu.VMEM((2 * pts, pts), f32),
            pltpu.VMEM((2 * pts, feat), f32),
            pltpu.VMEM((2 * pts, feat), f32),
            pltpu.VMEM((2 * pts, feat), bf),
            pltpu.VMEM((n_q, share, feat), bf),
            pltpu.VMEM((n_q, share, feat), bf),
            pltpu.VMEM((n_q, share, feat), bf),
            pltpu.VMEM((n_q, share, feat), bf),
            pltpu.VMEM((share, feat), bf),
            pltpu.VMEM((share, feat), bf),
            dma((4, 2, slots)),
            dma((2, slots)),
            dma((4,)),
            dma((4,)),
            dma((n_q,)),
            dma((n_q,)),
            dma((n_q,)),
            dma((n_q,)),
            dma,
            dma,
        ],
        compiler_params=pltpu.CompilerParams(
            collective_id=0, has_side_effects=True, vmem_limit_bytes=32 * 1024 * 1024
        ),
    )(hidden, projection, fac, amplitude, length_sq)


def per_shard(n_row, n_col, hidden, projection, alpha, probe_pairs, amplitude, length_sq):
    pts, hid = hidden.shape
    feat = projection.shape[1]
    probes = probe_pairs.shape[1] // 2
    fits = (
        n_row % 4 == 0
        and n_col == 2
        and n_row * n_col <= 64
        and pts == LANES
        and feat % LANES == 0
        and feat >= 3 * pts
        and probes == TILE
        and hid % (n_row * TILE) == 0
    )
    args = (hidden, projection, alpha, probe_pairs, amplitude, length_sq)
    if fits:
        return fused(n_row, n_col, *args)
    return per_device(*args)


def solution(mesh):
    placed = (P(("row", "col"), None), P(), P(("row", "col")), P(("row", "col"), None), P(), P())
    return jax.shard_map(
        functools.partial(per_shard, mesh.shape["row"], mesh.shape["col"]),
        mesh=mesh,
        in_specs=placed,
        out_specs=(P(("row", "col"), None), P("row", None)),
        check_vma=False,
    )
```

```python
import functools
import math

import jax
import jax.numpy as jnp
from jax import lax
from jax.experimental import pallas as pl
from jax.experimental.pallas import tpu as pltpu
from jax.sharding import PartitionSpec as P


def right_of(factors, probes):
    scale = 1.0 / (4 * probes)
    return jnp.concatenate(
        [
            factors[:, :1] * 0.5,
            factors[:, 1 + probes :] * -scale,
            factors[:, 1 : 1 + probes] * -scale,
        ],
        axis=1,
    )


def squares(feats):
    feat_f = feats.astype(jnp.float32)
    return jnp.sum(feat_f * feat_f, axis=1)


def per_device(hidden, projection, alpha, probe_pairs, amplitude, length_sq):
    feats = jnp.dot(hidden, projection, preferred_element_type=jnp.float32).astype(jnp.bfloat16)
    factors = jnp.concatenate([alpha[:, None], probe_pairs], axis=1)
    probes = probe_pairs.shape[1] // 2
    amp = amplitude[0]
    lsq = length_sq[0]
    width = feats.shape[1]

    def make_fold(rows_feat, rows_fac):
        rows_sq = squares(rows_feat)

        def fold(carry, pieces, start):
            cols_feat, cols_fac = pieces
            count = cols_feat.shape[0]
            size = math.gcd(count, 256)
            steps_feat = cols_feat.reshape(count // size, size, width)
            steps_fac = cols_fac.reshape(count // size, size, cols_fac.shape[1])

            def inner_step(state, blocks):
                block_feat, block_fac = blocks
                moved, rowsum = state
                block_sq = squares(block_feat)
                inner = jnp.dot(rows_feat, block_feat.T, preferred_element_type=jnp.float32)
                dist = rows_sq[:, None] + block_sq[None, :] - 2.0 * inner
                kern = amp * jnp.exp(-0.5 * dist / lsq)
                gmat = jnp.dot(
                    rows_fac, right_of(block_fac, probes).T, preferred_element_type=jnp.float32
                )
                weight = gmat * kern
                rowsum = rowsum + jnp.sum(weight, axis=1)
                moved = moved + jnp.dot(
                    weight.astype(jnp.bfloat16), block_feat, preferred_element_type=jnp.float32
                )
                return ((moved, rowsum), None)

            result, unused = lax.scan(inner_step, carry, (steps_feat, steps_fac))
            return result

        start_carry = (
            jnp.zeros((rows_feat.shape[0], width), jnp.float32),
            jnp.zeros((rows_feat.shape[0],), jnp.float32),
        )
        return (fold, start_carry)

    rows_feat, rows_fac = (
        lax.all_gather(feats, "row", axis=0, tiled=True),
        lax.all_gather(factors, "row", axis=0, tiled=True),
    )
    fold, start_carry = make_fold(rows_feat, rows_fac)
    moved, rowsum = fold(
        start_carry,
        (
            lax.all_gather(feats, "col", axis=0, tiled=True),
            lax.all_gather(factors, "col", axis=0, tiled=True),
        ),
        jnp.int32(0),
    )
    moved_own, rowsum_own = (
        lax.psum_scatter(moved, "row", scatter_dimension=0, tiled=True),
        lax.psum_scatter(rowsum, "row", scatter_dimension=0, tiled=True),
    )
    grad_feat = (2.0 / lsq * (moved_own - rowsum_own[:, None] * feats.astype(jnp.float32))).astype(
        jnp.bfloat16
    )
    grad_hidden = jnp.dot(grad_feat, projection.T, preferred_element_type=jnp.float32).astype(
        jnp.bfloat16
    )
    partial_proj = lax.dot_general(
        hidden, grad_feat, (((0,), (0,)), ((), ())), preferred_element_type=jnp.float32
    )
    share = lax.psum_scatter(
        partial_proj.astype(jnp.bfloat16), "row", scatter_dimension=0, tiled=True
    )
    grad_proj = lax.psum(share, "col").astype(jnp.float32)
    return (grad_hidden, grad_proj)


TILE = 16
LANES = 128
ROUTES = ("qcy", "qyc", "ycq")
FIRST_SENDS = ("2y", "0c", "0q", "1q", "1y", "2c", "0y", "1c", "2q")
MESH = pl.DeviceIdType.MESH
NT = (((1,), (1,)), ((), ()))


def fused_kernel(
    n_q,
    hidden_hbm,
    proj_hbm,
    pairs_hbm,
    alpha_ref,
    amp,
    lsq,
    gh_ref,
    gp_ref,
    blocks,
    rows_blk,
    rows_fac,
    rows_hid,
    hidden,
    proj,
    pairs,
    row_sq,
    hid_t,
    moved,
    rowsum,
    part_d,
    peer_d,
    grad,
    y_out,
    y_in,
    q_out,
    q_in,
    x_out,
    x_in,
    send_sems,
    recv_sems,
    core_send,
    core_recv,
    y_send,
    y_recv,
    q_send,
    q_recv,
    x_send,
    x_recv,
    load_sems,
):
    loads = [
        pltpu.make_async_copy(src, dst, load_sems.at[i])
        for i, (src, dst) in enumerate(
            ((proj_hbm, proj), (hidden_hbm, hidden), (pairs_hbm, pairs))
        )
    ]
    for load in loads:
        load.start()
    r = lax.axis_index("row")
    c = lax.axis_index("col")
    k = lax.rem(r, 2)
    y = lax.rem(r // 2, 2)
    q = r // 4
    pts, hid = hidden.shape
    feat = proj.shape[1]
    share = gp_ref.shape[0]
    probes = pairs.shape[1] // 2
    step_scale = 1.0 / (4 * probes)

    def dev(qq, yy, cc, kk):
        return ((qq * 2 + yy) * 2 + kk, cc)

    y_nbr = dev(q, 1 - y, c, k)
    c_nbr = dev(q, y, 1 - c, k)
    core = dev(q, y, c, 1 - k)
    q_up = dev(jnp.minimum(q + 1, n_q - 1), y, c, k)
    q_dn = dev(jnp.maximum(q - 1, 0), y, c, k)

    barrier = pltpu.get_barrier_semaphore()
    for nbr in (y_nbr, c_nbr, core):
        pl.semaphore_signal(barrier, inc=1, device_id=nbr, device_id_type=MESH)
    for i in range(1, n_q):
        pl.semaphore_signal(
            barrier, inc=1, device_id=dev(lax.rem(q + i, n_q), y, c, k), device_id_type=MESH
        )

    def slot_of(oq, oy, oc):
        return (oq * 2 + oy) * 2 + oc

    mine = slot_of(q, y, c)

    for load in loads:
        load.wait()

    feats = jnp.dot(hidden[...], proj[...], preferred_element_type=jnp.float32).astype(jnp.bfloat16)
    feat_f = feats.astype(jnp.float32)
    sq = lax.dot_general(
        jnp.ones((8, feat), jnp.float32),
        feat_f * feat_f,
        NT,
        precision=lax.Precision.HIGHEST,
        preferred_element_type=jnp.float32,
    )
    sq = jnp.concatenate([sq, sq], axis=0)
    hi = sq.astype(jnp.bfloat16).astype(jnp.float32)
    mi = (sq - hi).astype(jnp.bfloat16).astype(jnp.float32)
    lo = sq - hi - mi
    eye = lax.broadcasted_iota(jnp.int32, (2 * probes, 2 * probes), 0)
    eye = (eye == lax.broadcasted_iota(jnp.int32, (2 * probes, 2 * probes), 1)).astype(jnp.bfloat16)
    pairs_t = lax.dot_general(eye, pairs[...], NT, preferred_element_type=jnp.float32)
    place = lax.broadcasted_iota(jnp.int32, (TILE, pts), 0)
    last = jnp.where(
        place == 0, jnp.broadcast_to(alpha_ref[...].astype(jnp.float32), (TILE, pts)), 0.0
    )
    last = jnp.where(place == 1, hi, jnp.where(place == 2, mi, jnp.where(place == 3, lo, last)))
    blocks[mine, 0:pts, :] = feats
    blocks[mine, pts:, 3 * pts :] = jnp.zeros((TILE, feat - 3 * pts), jnp.bfloat16)
    blocks[mine, pts:, 0:pts] = pairs_t[0:TILE].astype(jnp.bfloat16)
    blocks[mine, pts:, pts : 2 * pts] = pairs_t[TILE : 2 * TILE].astype(jnp.bfloat16)
    blocks[mine, pts:, 2 * pts : 3 * pts] = last.astype(jnp.bfloat16)
    rows_blk[k] = blocks[mine]

    pl.semaphore_wait(barrier, 3 + n_q - 1)

    def to_core(index, src, dst):
        return pltpu.make_async_remote_copy(
            src_ref=src,
            dst_ref=dst,
            send_sem=core_send.at[index],
            recv_sem=core_recv.at[index],
            device_id=core,
            device_id_type=MESH,
        )

    first = (to_core(0, blocks.at[mine], rows_blk.at[k]), to_core(2, hidden, rows_hid))

    cut = (pts // 4, 5 * pts // 8)
    spans = ((cut[1], pts + TILE - cut[1]), (cut[0], cut[1] - cut[0]), (0, cut[0]))

    def hop(direction, part, slot, nbr):
        piece = blocks.at[slot, pl.ds(*spans[part])]
        return pltpu.make_async_remote_copy(
            src_ref=piece,
            dst_ref=piece,
            send_sem=send_sems.at[direction, part, slot],
            recv_sem=recv_sems.at[part, slot],
            device_id=nbr,
            device_id_type=MESH,
        )

    sent = []

    def send(pred, copy):
        sent.append((pred, copy))
        if pred is None:
            copy.start()
        else:
            pl.when(pred)(copy.start)

    def both(a, b):
        return b if a is None else jnp.logical_and(a, b)

    def send_along(dim, exists, part, oq, slot):
        if dim == "y":
            send(exists, hop(2, part, slot, y_nbr))
        elif dim == "c":
            send(exists, hop(3, part, slot, c_nbr))
        else:
            up = jnp.logical_and(oq <= q, q + 1 < n_q)
            down = jnp.logical_and(oq >= q, q > 0)
            send(both(exists, up), hop(0, part, slot, q_up))
            send(both(exists, down), hop(1, part, slot, q_dn))

    def forward(exists, part, oq, dq, iy, ic):
        slot = slot_of(oq, (y + iy) % 2, (c + ic) % 2)
        pl.when(exists)(hop(0, part, slot, y_nbr).wait_recv)
        apart = {"q": dq, "y": iy, "c": ic}
        route = ROUTES[part]
        latest = max(at for at, dim in enumerate(route) if apart[dim])
        for at, dim in enumerate(route):
            if at > latest or (at == latest and dim == "q"):
                send_along(dim, exists, part, oq, slot)

    scale = -0.5 / lsq[0]

    def fold(slot):
        blk = blocks[slot, 0:pts, :]
        aux = blocks[slot, pts:, :]
        rows = jnp.concatenate([rows_blk[0, 0:pts], rows_blk[1, 0:pts]], axis=0)
        inner = lax.dot_general(rows, blk, NT, preferred_element_type=jnp.float32)
        tail = aux[:, 2 * pts : 3 * pts].astype(jnp.float32)
        col_sq = tail[1:2] + tail[2:3] + tail[3:4]
        dist = row_sq[...] + col_sq - 2.0 * inner
        kern = jnp.exp(dist * scale)
        col_fac = jnp.concatenate(
            [
                aux[:, 0:pts],
                aux[:, pts : 2 * pts],
                aux[:, 2 * pts : 3 * pts],
                jnp.zeros((LANES - 3 * TILE, pts), jnp.bfloat16),
            ],
            axis=0,
        )
        lefts = rows_fac[...]
        gmat = jnp.dot(lefts, col_fac, preferred_element_type=jnp.float32)
        weight = gmat * kern
        rowsum[...] += weight
        moved[...] += jnp.dot(weight.astype(jnp.bfloat16), blk, preferred_element_type=jnp.float32)

    def fold_level(level):
        def step(e, carry):
            iy, ic, side = e // 4, lax.rem(e // 2, 2), lax.rem(e, 2)
            dq = level - iy - ic
            oq = q + dq * (1 - 2 * side)
            good = (dq >= 0) & (dq < n_q) & (oq >= 0) & (oq < n_q) & ((dq > 0) | (side == 0))

            @pl.when(good)
            def _():
                fold(slot_of(oq, lax.rem(y + iy, 2), lax.rem(c + ic, 2)))

            return carry

        lax.fori_loop(0, 8, step, 0)

    def arrivals(level):
        for iy, ic in ((0, 0), (0, 1), (1, 0), (1, 1)):
            dq = level - iy - ic
            if dq < 0 or dq >= n_q:
                continue
            for side in (1, -1) if dq else (1,):
                oq = q + side * dq
                exists = jnp.logical_and(oq >= 0, oq < n_q)
                for part in range(len(ROUTES)):
                    forward(exists, part, oq, dq, iy, ic)

    for first_send in FIRST_SENDS:
        send_along(first_send[1], None, int(first_send[0]), q, mine)
    for copy in first:
        copy.start()
    moved[...] = jnp.zeros_like(moved)
    rowsum[...] = jnp.zeros_like(rowsum)
    for copy in first:
        copy.wait_recv()
    for half in range(2):
        f = rows_blk[half, 0:pts].astype(jnp.float32)
        span = slice(half * pts, (half + 1) * pts)
        row_sq[span, :] = jnp.broadcast_to(jnp.sum(f * f, axis=1, keepdims=True), (pts, pts))
        aux = rows_blk[half, pts:, 0 : 3 * pts].astype(jnp.float32)
        left_t = jnp.concatenate(
            [
                aux[:, pts : 2 * pts] * -step_scale,
                aux[:, 0:pts] * -step_scale,
                jnp.where(place == 0, aux[:, 2 * pts :] * 0.5, 0.0),
                jnp.zeros((LANES - 3 * TILE, pts), jnp.float32),
            ],
            axis=0,
        )
        rows_fac[span, :] = left_t.T.astype(jnp.bfloat16)

    for level in range(n_q + 2):
        if level + 1 < n_q + 1:
            arrivals(level + 1)
        if level == n_q + 1:
            arrivals(level)
        if level == 1:
            own_t = hidden[...].astype(jnp.float32).T.astype(jnp.bfloat16)
            peer_t = rows_hid[...].astype(jnp.float32).T.astype(jnp.bfloat16)
            low = k == 0
            hid_t[:, 0:pts] = jnp.where(low, own_t, peer_t)
            hid_t[:, pts:] = jnp.where(low, peer_t, own_t)
        fold_level(level)

    rows_f = jnp.concatenate([rows_blk[0, 0:pts], rows_blk[1, 0:pts]], axis=0).astype(jnp.float32)
    part_d[...] = moved[...] - jnp.sum(rowsum[...], axis=1, keepdims=True) * rows_f
    swap = to_core(3, part_d, peer_d)
    swap.start()
    swap.wait_recv()
    grad[...] = ((2.0 * amp[0] / lsq[0]) * (part_d[...] + peer_d[...])).astype(jnp.bfloat16)

    def term(qj, yj):
        start = pl.multiple_of(((qj * 2 + yj) * 2 + k) * share, TILE)
        return jnp.dot(hid_t[pl.ds(start, share), :], grad[...], preferred_element_type=jnp.float32)

    def to_y(qj):
        return pltpu.make_async_remote_copy(
            src_ref=y_out.at[qj],
            dst_ref=y_in.at[qj],
            send_sem=y_send.at[qj],
            recv_sem=y_recv.at[qj],
            device_id=y_nbr,
            device_id_type=MESH,
        )

    def to_q(qj):
        return pltpu.make_async_remote_copy(
            src_ref=q_out.at[qj],
            dst_ref=q_in.at[q],
            send_sem=q_send.at[qj],
            recv_sem=q_recv.at[q],
            device_id=dev(qj, y, c, k),
            device_id_type=MESH,
        )

    def from_q(qj):
        return pltpu.make_async_remote_copy(
            src_ref=q_out.at[qj],
            dst_ref=q_in.at[qj],
            send_sem=q_send.at[qj],
            recv_sem=q_recv.at[qj],
            device_id=dev(qj, y, c, k),
            device_id_type=MESH,
        )

    order = []
    for i in range(n_q - 1):
        rising = jnp.where(i >= q, i + 1, i)
        falling = jnp.where(n_q - 1 - i <= q, n_q - 2 - i, n_q - 1 - i)
        order.append(jnp.where(2 * q < n_q, falling, rising))
    order.append(q)
    for qj in order:
        y_out[qj] = term(qj, 1 - y).astype(jnp.bfloat16)
        to_y(qj).start()
    own_rows = grad[pl.ds(pl.multiple_of(k * pts, pts), pts), :]
    gh_ref[...] = lax.dot_general(
        own_rows, proj[...], NT, preferred_element_type=jnp.float32
    ).astype(jnp.bfloat16)
    total = None
    for qj in order:
        own_term = term(qj, y)
        to_y(qj).wait_recv()
        summed = own_term + y_in[qj].astype(jnp.float32)
        if qj is order[-1]:
            total = summed
        else:
            q_out[qj] = summed.astype(jnp.bfloat16)
            to_q(qj).start()
    for qj in order[:-1]:
        from_q(qj).wait_recv()
        total = total + q_in[qj].astype(jnp.float32)
    x_out[...] = total.astype(jnp.bfloat16)
    to_x = pltpu.make_async_remote_copy(
        src_ref=x_out,
        dst_ref=x_in,
        send_sem=x_send,
        recv_sem=x_recv,
        device_id=c_nbr,
        device_id_type=MESH,
    )
    to_x.start()
    to_x.wait_recv()
    gp_ref[...] = x_out[...].astype(jnp.float32) + x_in[...].astype(jnp.float32)

    for pred, copy in sent:
        if pred is None:
            copy.wait_send()
        else:
            pl.when(pred)(copy.wait_send)
    for copy in first:
        copy.wait_send()
    swap.wait_send()
    for qj in order:
        to_y(qj).wait_send()
    for qj in order[:-1]:
        to_q(qj).wait_send()
    to_x.wait_send()


def fused(n_row, n_col, hidden, projection, alpha, probe_pairs, amplitude, length_sq):
    pts, hid = hidden.shape
    feat = projection.shape[1]
    probes = probe_pairs.shape[1] // 2
    slots = n_row * n_col // 2
    n_q = n_row // 4
    share = hid // n_row
    vmem = pl.BlockSpec(memory_space=pltpu.VMEM)
    hbm = pl.BlockSpec(memory_space=pl.ANY)
    smem = pl.BlockSpec(memory_space=pltpu.SMEM)
    bf, f32 = jnp.bfloat16, jnp.float32
    dma = pltpu.SemaphoreType.DMA
    return pl.pallas_call(
        functools.partial(fused_kernel, n_q),
        out_shape=(
            jax.ShapeDtypeStruct((pts, hid), bf),
            jax.ShapeDtypeStruct((share, feat), f32),
        ),
        in_specs=[hbm, hbm, hbm, vmem, smem, smem],
        out_specs=(vmem, vmem),
        scratch_shapes=[
            pltpu.VMEM((slots, pts + TILE, feat), bf),
            pltpu.VMEM((2, pts + TILE, feat), bf),
            pltpu.VMEM((2 * pts, LANES), bf),
            pltpu.VMEM((pts, hid), bf),
            pltpu.VMEM((pts, hid), bf),
            pltpu.VMEM((hid, feat), bf),
            pltpu.VMEM((pts, 2 * probes), bf),
            pltpu.VMEM((2 * pts, pts), f32),
            pltpu.VMEM((hid, 2 * pts), bf),
            pltpu.VMEM((2 * pts, feat), f32),
            pltpu.VMEM((2 * pts, pts), f32),
            pltpu.VMEM((2 * pts, feat), f32),
            pltpu.VMEM((2 * pts, feat), f32),
            pltpu.VMEM((2 * pts, feat), bf),
            pltpu.VMEM((n_q, share, feat), bf),
            pltpu.VMEM((n_q, share, feat), bf),
            pltpu.VMEM((n_q, share, feat), bf),
            pltpu.VMEM((n_q, share, feat), bf),
            pltpu.VMEM((share, feat), bf),
            pltpu.VMEM((share, feat), bf),
            dma((4, len(ROUTES), slots)),
            dma((len(ROUTES), slots)),
            dma((4,)),
            dma((4,)),
            dma((n_q,)),
            dma((n_q,)),
            dma((n_q,)),
            dma((n_q,)),
            dma,
            dma,
            dma((3,)),
        ],
        compiler_params=pltpu.CompilerParams(
            collective_id=0, has_side_effects=True, vmem_limit_bytes=32 * 1024 * 1024
        ),
    )(hidden, projection, probe_pairs, alpha[None, :], amplitude, length_sq)


def per_shard(n_row, n_col, hidden, projection, alpha, probe_pairs, amplitude, length_sq):
    pts, hid = hidden.shape
    feat = projection.shape[1]
    probes = probe_pairs.shape[1] // 2
    fits = (
        n_row % 4 == 0
        and n_col == 2
        and n_row * n_col <= 64
        and pts == LANES
        and feat % LANES == 0
        and feat >= 3 * pts
        and probes == TILE
        and hid % (n_row * TILE) == 0
    )
    args = (hidden, projection, alpha, probe_pairs, amplitude, length_sq)
    if fits:
        return fused(n_row, n_col, *args)
    return per_device(*args)


def solution(mesh):
    placed = (P(("row", "col"), None), P(), P(("row", "col")), P(("row", "col"), None), P(), P())
    return jax.shard_map(
        functools.partial(per_shard, mesh.shape["row"], mesh.shape["col"]),
        mesh=mesh,
        in_specs=placed,
        out_specs=(P(("row", "col"), None), P("row", None)),
        check_vma=False,
    )
```

```python
import functools
import math

import jax
import jax.numpy as jnp
from jax import lax
from jax.experimental import pallas as pl
from jax.experimental.pallas import tpu as pltpu
from jax.sharding import PartitionSpec as P


def right_of(factors, probes):
    scale = 1.0 / (4 * probes)
    return jnp.concatenate(
        [
            factors[:, :1] * 0.5,
            factors[:, 1 + probes :] * -scale,
            factors[:, 1 : 1 + probes] * -scale,
        ],
        axis=1,
    )


def squares(feats):
    feat_f = feats.astype(jnp.float32)
    return jnp.sum(feat_f * feat_f, axis=1)


def per_device(hidden, projection, alpha, probe_pairs, amplitude, length_sq):
    feats = jnp.dot(hidden, projection, preferred_element_type=jnp.float32).astype(jnp.bfloat16)
    factors = jnp.concatenate([alpha[:, None], probe_pairs], axis=1)
    probes = probe_pairs.shape[1] // 2
    amp = amplitude[0]
    lsq = length_sq[0]
    width = feats.shape[1]

    def make_fold(rows_feat, rows_fac):
        rows_sq = squares(rows_feat)

        def fold(carry, pieces, start):
            cols_feat, cols_fac = pieces
            count = cols_feat.shape[0]
            size = math.gcd(count, 256)
            steps_feat = cols_feat.reshape(count // size, size, width)
            steps_fac = cols_fac.reshape(count // size, size, cols_fac.shape[1])

            def inner_step(state, blocks):
                block_feat, block_fac = blocks
                moved, rowsum = state
                block_sq = squares(block_feat)
                inner = jnp.dot(rows_feat, block_feat.T, preferred_element_type=jnp.float32)
                dist = rows_sq[:, None] + block_sq[None, :] - 2.0 * inner
                kern = amp * jnp.exp(-0.5 * dist / lsq)
                gmat = jnp.dot(
                    rows_fac, right_of(block_fac, probes).T, preferred_element_type=jnp.float32
                )
                weight = gmat * kern
                rowsum = rowsum + jnp.sum(weight, axis=1)
                moved = moved + jnp.dot(
                    weight.astype(jnp.bfloat16), block_feat, preferred_element_type=jnp.float32
                )
                return ((moved, rowsum), None)

            result, unused = lax.scan(inner_step, carry, (steps_feat, steps_fac))
            return result

        start_carry = (
            jnp.zeros((rows_feat.shape[0], width), jnp.float32),
            jnp.zeros((rows_feat.shape[0],), jnp.float32),
        )
        return (fold, start_carry)

    rows_feat, rows_fac = (
        lax.all_gather(feats, "row", axis=0, tiled=True),
        lax.all_gather(factors, "row", axis=0, tiled=True),
    )
    fold, start_carry = make_fold(rows_feat, rows_fac)
    moved, rowsum = fold(
        start_carry,
        (
            lax.all_gather(feats, "col", axis=0, tiled=True),
            lax.all_gather(factors, "col", axis=0, tiled=True),
        ),
        jnp.int32(0),
    )
    moved_own, rowsum_own = (
        lax.psum_scatter(moved, "row", scatter_dimension=0, tiled=True),
        lax.psum_scatter(rowsum, "row", scatter_dimension=0, tiled=True),
    )
    grad_feat = (2.0 / lsq * (moved_own - rowsum_own[:, None] * feats.astype(jnp.float32))).astype(
        jnp.bfloat16
    )
    grad_hidden = jnp.dot(grad_feat, projection.T, preferred_element_type=jnp.float32).astype(
        jnp.bfloat16
    )
    partial_proj = lax.dot_general(
        hidden, grad_feat, (((0,), (0,)), ((), ())), preferred_element_type=jnp.float32
    )
    share = lax.psum_scatter(
        partial_proj.astype(jnp.bfloat16), "row", scatter_dimension=0, tiled=True
    )
    grad_proj = lax.psum(share, "col").astype(jnp.float32)
    return (grad_hidden, grad_proj)


TILE = 16
LANES = 128
ROUTES = ("qcy", "qyc", "ycq")
FIRST_SENDS = ("2y", "0c", "0q", "1q", "1y", "2c", "0y", "1c", "2q")
MESH = pl.DeviceIdType.MESH
NT = (((1,), (1,)), ((), ()))


def fused_kernel(
    n_q,
    hidden_hbm,
    proj_hbm,
    pairs_hbm,
    alpha_ref,
    amp,
    lsq,
    gh_ref,
    gp_ref,
    blocks,
    rows_blk,
    rows_fac,
    rows_hid,
    hidden,
    proj,
    pairs,
    row_sq,
    hid_t,
    moved,
    rowsum,
    part_d,
    peer_d,
    grad,
    y_out,
    y_in,
    q_out,
    q_in,
    x_out,
    x_in,
    send_sems,
    recv_sems,
    core_send,
    core_recv,
    y_send,
    y_recv,
    q_send,
    q_recv,
    x_send,
    x_recv,
    load_sems,
):
    loads = [
        pltpu.make_async_copy(src, dst, load_sems.at[i])
        for i, (src, dst) in enumerate(
            ((proj_hbm, proj), (hidden_hbm, hidden), (pairs_hbm, pairs))
        )
    ]
    for load in loads:
        load.start()
    r = lax.axis_index("row")
    c = lax.axis_index("col")
    k = lax.rem(r, 2)
    y = lax.rem(r // 2, 2)
    q = r // 4
    pts, hid = hidden.shape
    feat = proj.shape[1]
    share = gp_ref.shape[0]
    probes = pairs.shape[1] // 2
    step_scale = 1.0 / (4 * probes)

    def dev(qq, yy, cc, kk):
        return ((qq * 2 + yy) * 2 + kk, cc)

    y_nbr = dev(q, 1 - y, c, k)
    c_nbr = dev(q, y, 1 - c, k)
    core = dev(q, y, c, 1 - k)
    q_up = dev(jnp.minimum(q + 1, n_q - 1), y, c, k)
    q_dn = dev(jnp.maximum(q - 1, 0), y, c, k)

    barrier = pltpu.get_barrier_semaphore()
    for nbr in (y_nbr, c_nbr, core):
        pl.semaphore_signal(barrier, inc=1, device_id=nbr, device_id_type=MESH)
    for i in range(1, n_q):
        pl.semaphore_signal(
            barrier, inc=1, device_id=dev(lax.rem(q + i, n_q), y, c, k), device_id_type=MESH
        )

    def slot_of(oq, oy, oc):
        return (oq * 2 + oy) * 2 + oc

    mine = slot_of(q, y, c)

    for load in loads:
        load.wait()

    feats = jnp.dot(hidden[...], proj[...], preferred_element_type=jnp.float32).astype(jnp.bfloat16)
    feat_f = feats.astype(jnp.float32)
    sq = lax.dot_general(
        jnp.ones((8, feat), jnp.float32),
        feat_f * feat_f,
        NT,
        precision=lax.Precision.HIGHEST,
        preferred_element_type=jnp.float32,
    )
    sq = jnp.concatenate([sq, sq], axis=0)
    hi = sq.astype(jnp.bfloat16).astype(jnp.float32)
    mi = (sq - hi).astype(jnp.bfloat16).astype(jnp.float32)
    lo = sq - hi - mi
    eye = lax.broadcasted_iota(jnp.int32, (2 * probes, 2 * probes), 0)
    eye = (eye == lax.broadcasted_iota(jnp.int32, (2 * probes, 2 * probes), 1)).astype(jnp.bfloat16)
    pairs_t = lax.dot_general(eye, pairs[...], NT, preferred_element_type=jnp.float32)
    place = lax.broadcasted_iota(jnp.int32, (TILE, pts), 0)
    last = jnp.where(
        place == 0, jnp.broadcast_to(alpha_ref[...].astype(jnp.float32), (TILE, pts)), 0.0
    )
    last = jnp.where(place == 1, hi, jnp.where(place == 2, mi, jnp.where(place == 3, lo, last)))
    blocks[mine, 0:pts, :] = feats
    blocks[mine, pts:, 3 * pts :] = jnp.zeros((TILE, feat - 3 * pts), jnp.bfloat16)
    blocks[mine, pts:, 0:pts] = pairs_t[0:TILE].astype(jnp.bfloat16)
    blocks[mine, pts:, pts : 2 * pts] = pairs_t[TILE : 2 * TILE].astype(jnp.bfloat16)
    blocks[mine, pts:, 2 * pts : 3 * pts] = last.astype(jnp.bfloat16)
    rows_blk[k] = blocks[mine]

    pl.semaphore_wait(barrier, 3 + n_q - 1)

    def to_core(index, src, dst):
        return pltpu.make_async_remote_copy(
            src_ref=src,
            dst_ref=dst,
            send_sem=core_send.at[index],
            recv_sem=core_recv.at[index],
            device_id=core,
            device_id_type=MESH,
        )

    first = (to_core(0, blocks.at[mine], rows_blk.at[k]), to_core(2, hidden, rows_hid))

    cut = (pts // 4, 5 * pts // 8)
    spans = ((cut[1], pts + TILE - cut[1]), (cut[0], cut[1] - cut[0]), (0, cut[0]))

    def hop(direction, part, slot, nbr):
        piece = blocks.at[slot, pl.ds(*spans[part])]
        return pltpu.make_async_remote_copy(
            src_ref=piece,
            dst_ref=piece,
            send_sem=send_sems.at[direction, part, slot],
            recv_sem=recv_sems.at[part, slot],
            device_id=nbr,
            device_id_type=MESH,
        )

    sent = []

    def send(pred, copy):
        sent.append((pred, copy))
        if pred is None:
            copy.start()
        else:
            pl.when(pred)(copy.start)

    def both(a, b):
        return b if a is None else jnp.logical_and(a, b)

    def send_along(dim, exists, part, oq, slot):
        if dim == "y":
            send(exists, hop(2, part, slot, y_nbr))
        elif dim == "c":
            send(exists, hop(3, part, slot, c_nbr))
        else:
            up = jnp.logical_and(oq <= q, q + 1 < n_q)
            down = jnp.logical_and(oq >= q, q > 0)
            send(both(exists, up), hop(0, part, slot, q_up))
            send(both(exists, down), hop(1, part, slot, q_dn))

    def forward(exists, part, oq, dq, iy, ic):
        slot = slot_of(oq, (y + iy) % 2, (c + ic) % 2)
        pl.when(exists)(hop(0, part, slot, y_nbr).wait_recv)
        apart = {"q": dq, "y": iy, "c": ic}
        route = ROUTES[part]
        latest = max(at for at, dim in enumerate(route) if apart[dim])
        for at, dim in enumerate(route):
            if at > latest or (at == latest and dim == "q"):
                send_along(dim, exists, part, oq, slot)

    scale = -0.5 / lsq[0]

    def fold(slot):
        blk = blocks[slot, 0:pts, :]
        aux = blocks[slot, pts:, :]
        rows = jnp.concatenate([rows_blk[0, 0:pts], rows_blk[1, 0:pts]], axis=0)
        inner = lax.dot_general(rows, blk, NT, preferred_element_type=jnp.float32)
        tail = aux[:, 2 * pts : 3 * pts].astype(jnp.float32)
        col_sq = tail[1:2] + tail[2:3] + tail[3:4]
        dist = row_sq[...] + col_sq - 2.0 * inner
        kern = jnp.exp(dist * scale)
        col_fac = jnp.concatenate(
            [
                aux[:, 0:pts],
                aux[:, pts : 2 * pts],
                aux[:, 2 * pts : 3 * pts],
                jnp.zeros((LANES - 3 * TILE, pts), jnp.bfloat16),
            ],
            axis=0,
        )
        lefts = rows_fac[...]
        gmat = jnp.dot(lefts, col_fac, preferred_element_type=jnp.float32)
        weight = gmat * kern
        rowsum[...] += weight
        moved[...] += jnp.dot(weight.astype(jnp.bfloat16), blk, preferred_element_type=jnp.float32)

    def fold_level(level):
        def step(e, carry):
            iy, ic, side = e // 4, lax.rem(e // 2, 2), lax.rem(e, 2)
            dq = level - iy - ic
            oq = q + dq * (1 - 2 * side)
            good = (dq >= 0) & (dq < n_q) & (oq >= 0) & (oq < n_q) & ((dq > 0) | (side == 0))

            @pl.when(good)
            def _():
                fold(slot_of(oq, lax.rem(y + iy, 2), lax.rem(c + ic, 2)))

            return carry

        lax.fori_loop(0, 8, step, 0)

    def arrivals(level):
        for iy, ic in ((0, 0), (0, 1), (1, 0), (1, 1)):
            dq = level - iy - ic
            if dq < 0 or dq >= n_q:
                continue
            for side in (1, -1) if dq else (1,):
                oq = q + side * dq
                exists = jnp.logical_and(oq >= 0, oq < n_q)
                for part in range(len(ROUTES)):
                    forward(exists, part, oq, dq, iy, ic)

    for first_send in FIRST_SENDS:
        send_along(first_send[1], None, int(first_send[0]), q, mine)
    for copy in first:
        copy.start()
    moved[...] = jnp.zeros_like(moved)
    rowsum[...] = jnp.zeros_like(rowsum)
    for copy in first:
        copy.wait_recv()
    for half in range(2):
        f = rows_blk[half, 0:pts].astype(jnp.float32)
        span = slice(half * pts, (half + 1) * pts)
        row_sq[span, :] = jnp.broadcast_to(jnp.sum(f * f, axis=1, keepdims=True), (pts, pts))
        aux = rows_blk[half, pts:, 0 : 3 * pts].astype(jnp.float32)
        left_t = jnp.concatenate(
            [
                aux[:, pts : 2 * pts] * -step_scale,
                aux[:, 0:pts] * -step_scale,
                jnp.where(place == 0, aux[:, 2 * pts :] * 0.5, 0.0),
                jnp.zeros((LANES - 3 * TILE, pts), jnp.float32),
            ],
            axis=0,
        )
        rows_fac[span, :] = left_t.T.astype(jnp.bfloat16)

    for level in range(n_q + 2):
        if level > 0:
            arrivals(level)
        if level == 1:
            own_t = hidden[...].astype(jnp.float32).T.astype(jnp.bfloat16)
            peer_t = rows_hid[...].astype(jnp.float32).T.astype(jnp.bfloat16)
            low = k == 0
            hid_t[:, 0:pts] = jnp.where(low, own_t, peer_t)
            hid_t[:, pts:] = jnp.where(low, peer_t, own_t)
        fold_level(level)

    rows_f = jnp.concatenate([rows_blk[0, 0:pts], rows_blk[1, 0:pts]], axis=0).astype(jnp.float32)
    part_d[...] = moved[...] - jnp.sum(rowsum[...], axis=1, keepdims=True) * rows_f
    swap = to_core(3, part_d, peer_d)
    swap.start()
    swap.wait_recv()
    grad[...] = ((2.0 * amp[0] / lsq[0]) * (part_d[...] + peer_d[...])).astype(jnp.bfloat16)

    def term(qj, yj):
        start = pl.multiple_of(((qj * 2 + yj) * 2 + k) * share, TILE)
        return jnp.dot(hid_t[pl.ds(start, share), :], grad[...], preferred_element_type=jnp.float32)

    def to_y(qj):
        return pltpu.make_async_remote_copy(
            src_ref=y_out.at[qj],
            dst_ref=y_in.at[qj],
            send_sem=y_send.at[qj],
            recv_sem=y_recv.at[qj],
            device_id=y_nbr,
            device_id_type=MESH,
        )

    def to_q(qj):
        return pltpu.make_async_remote_copy(
            src_ref=q_out.at[qj],
            dst_ref=q_in.at[q],
            send_sem=q_send.at[qj],
            recv_sem=q_recv.at[q],
            device_id=dev(qj, y, c, k),
            device_id_type=MESH,
        )

    def from_q(qj):
        return pltpu.make_async_remote_copy(
            src_ref=q_out.at[qj],
            dst_ref=q_in.at[qj],
            send_sem=q_send.at[qj],
            recv_sem=q_recv.at[qj],
            device_id=dev(qj, y, c, k),
            device_id_type=MESH,
        )

    order = []
    for i in range(n_q - 1):
        rising = jnp.where(i >= q, i + 1, i)
        falling = jnp.where(n_q - 1 - i <= q, n_q - 2 - i, n_q - 1 - i)
        order.append(jnp.where(2 * q < n_q, falling, rising))
    order.append(q)
    for qj in order:
        y_out[qj] = term(qj, 1 - y).astype(jnp.bfloat16)
        to_y(qj).start()
    own_rows = grad[pl.ds(pl.multiple_of(k * pts, pts), pts), :]
    gh_ref[...] = lax.dot_general(
        own_rows, proj[...], NT, preferred_element_type=jnp.float32
    ).astype(jnp.bfloat16)
    total = None
    for qj in order:
        own_term = term(qj, y)
        to_y(qj).wait_recv()
        summed = own_term + y_in[qj].astype(jnp.float32)
        if qj is order[-1]:
            total = summed
        else:
            q_out[qj] = summed.astype(jnp.bfloat16)
            to_q(qj).start()
    for qj in order[:-1]:
        from_q(qj).wait_recv()
        total = total + q_in[qj].astype(jnp.float32)
    x_out[...] = total.astype(jnp.bfloat16)
    to_x = pltpu.make_async_remote_copy(
        src_ref=x_out,
        dst_ref=x_in,
        send_sem=x_send,
        recv_sem=x_recv,
        device_id=c_nbr,
        device_id_type=MESH,
    )
    to_x.start()
    to_x.wait_recv()
    gp_ref[...] = x_out[...].astype(jnp.float32) + x_in[...].astype(jnp.float32)

    for pred, copy in sent:
        if pred is None:
            copy.wait_send()
        else:
            pl.when(pred)(copy.wait_send)
    for copy in first:
        copy.wait_send()
    swap.wait_send()
    for qj in order:
        to_y(qj).wait_send()
    for qj in order[:-1]:
        to_q(qj).wait_send()
    to_x.wait_send()


def fused(n_row, n_col, hidden, projection, alpha, probe_pairs, amplitude, length_sq):
    pts, hid = hidden.shape
    feat = projection.shape[1]
    probes = probe_pairs.shape[1] // 2
    slots = n_row * n_col // 2
    n_q = n_row // 4
    share = hid // n_row
    vmem = pl.BlockSpec(memory_space=pltpu.VMEM)
    hbm = pl.BlockSpec(memory_space=pl.ANY)
    smem = pl.BlockSpec(memory_space=pltpu.SMEM)
    bf, f32 = jnp.bfloat16, jnp.float32
    dma = pltpu.SemaphoreType.DMA
    return pl.pallas_call(
        functools.partial(fused_kernel, n_q),
        out_shape=(
            jax.ShapeDtypeStruct((pts, hid), bf),
            jax.ShapeDtypeStruct((share, feat), f32),
        ),
        in_specs=[hbm, hbm, hbm, vmem, smem, smem],
        out_specs=(vmem, vmem),
        scratch_shapes=[
            pltpu.VMEM((slots, pts + TILE, feat), bf),
            pltpu.VMEM((2, pts + TILE, feat), bf),
            pltpu.VMEM((2 * pts, LANES), bf),
            pltpu.VMEM((pts, hid), bf),
            pltpu.VMEM((pts, hid), bf),
            pltpu.VMEM((hid, feat), bf),
            pltpu.VMEM((pts, 2 * probes), bf),
            pltpu.VMEM((2 * pts, pts), f32),
            pltpu.VMEM((hid, 2 * pts), bf),
            pltpu.VMEM((2 * pts, feat), f32),
            pltpu.VMEM((2 * pts, pts), f32),
            pltpu.VMEM((2 * pts, feat), f32),
            pltpu.VMEM((2 * pts, feat), f32),
            pltpu.VMEM((2 * pts, feat), bf),
            pltpu.VMEM((n_q, share, feat), bf),
            pltpu.VMEM((n_q, share, feat), bf),
            pltpu.VMEM((n_q, share, feat), bf),
            pltpu.VMEM((n_q, share, feat), bf),
            pltpu.VMEM((share, feat), bf),
            pltpu.VMEM((share, feat), bf),
            dma((4, len(ROUTES), slots)),
            dma((len(ROUTES), slots)),
            dma((4,)),
            dma((4,)),
            dma((n_q,)),
            dma((n_q,)),
            dma((n_q,)),
            dma((n_q,)),
            dma,
            dma,
            dma((3,)),
        ],
        compiler_params=pltpu.CompilerParams(
            collective_id=0, has_side_effects=True, vmem_limit_bytes=62 * 1024 * 1024
        ),
    )(hidden, projection, probe_pairs, alpha[None, :], amplitude, length_sq)


def per_shard(n_row, n_col, hidden, projection, alpha, probe_pairs, amplitude, length_sq):
    pts, hid = hidden.shape
    feat = projection.shape[1]
    probes = probe_pairs.shape[1] // 2
    fits = (
        n_row % 4 == 0
        and n_col == 2
        and n_row * n_col <= 64
        and pts == LANES
        and feat % LANES == 0
        and feat >= 3 * pts
        and probes == TILE
        and hid % (n_row * TILE) == 0
    )
    args = (hidden, projection, alpha, probe_pairs, amplitude, length_sq)
    if fits:
        return fused(n_row, n_col, *args)
    return per_device(*args)


def solution(mesh):
    placed = (P(("row", "col"), None), P(), P(("row", "col")), P(("row", "col"), None), P(), P())
    return jax.shard_map(
        functools.partial(per_shard, mesh.shape["row"], mesh.shape["col"]),
        mesh=mesh,
        in_specs=placed,
        out_specs=(P(("row", "col"), None), P("row", None)),
        check_vma=False,
    )
```
